32 devices in a mesh: seq: 4 (over y, core), head: 8 (over z, x).
Axes of the slice: x: 2, y: 2, z: 4, core: 2. Of those that a mesh axis runs over, the one named last changes fastest.
Arguments:
- queries: bfloat16 [8, 2048, 256], P('head', 'seq'), may hold values from -6 to 6
- keys: bfloat16 [1, 2048, 256], P(None, 'seq'), may hold values from -6 to 6
- values: bfloat16 [1, 2048, 256], P(None, 'seq'), may hold values from -6 to 6
- d_out: bfloat16 [8, 2048, 256], P('head', 'seq'), may hold values from -12 to 12
- doc_lengths: int32 [1, 8], replicated, may hold values from 1 to 768, 2048 in all within a row
- fold_order: int32 [8], replicated, may hold values from 0 to 7, each once
Outputs:
- grad_queries: bfloat16 [8, 2048, 256], P('head', 'seq')
- grad_keys: float32 [1, 2048, 256], P(None, ('seq', 'head'))
- grad_values: float32 [1, 2048, 256], P(None, ('seq', 'head'))
The draws below stay inside these ranges and needn't reach their ends.
Inputs may be any that keep to these rules, and one draw needn't show every extreme that they name: `doc_lengths`: each row's 8 lengths are at least 1, sum to 2048, and the longest is exactly 768. fold_order names each of 0 to 7 once.
All inputs are finite; a program needn't handle non-finite values.
Results may differ from the reference program's by a relative error of at most 0.029.
Values may be sent and summed in bfloat16 or wider, within the bound.
No kernel may reach another device: no remote copies, remote signals or barrier semaphores. Data moves between devices by JAX's collectives and lax.ppermute only.
A program may use at most 64 MiB of HBM per device.

```python
import math
import jax
import jax.numpy as jnp
import numpy as np

HEAD_COUNT = 8
HEAD_DIM = 256
DOC_COUNT = 8
SEQ_LEN = 2048
BLOCK_LEN = 256
BLOCK_COUNT = 8
PACKED_ROWS = 1
ROW_HEADS = 8
DOC_MOST = 768


def draw_queries(key, part):
    full_shape = (ROW_HEADS, SEQ_LEN, HEAD_DIM)
    drawn = jnp.clip(jax.random.normal(jax.random.fold_in(key, 3), full_shape, jnp.float32), -6.0, 6.0)
    return drawn.astype(jnp.bfloat16)


def draw_keys(key, part):
    full_shape = (PACKED_ROWS, SEQ_LEN, HEAD_DIM)
    drawn = jnp.clip(jax.random.normal(jax.random.fold_in(key, 5), full_shape, jnp.float32), -6.0, 6.0)
    return drawn.astype(jnp.bfloat16)


def block_levels(key, dims, pieces, smallest, largest):
    factor_of, own = 1.0, jax.random.fold_in(key, 6)
    for dim, blocks in pieces:
        heights = jnp.exp(jax.random.uniform(jax.random.fold_in(own, dim), (blocks,), jnp.float32, smallest / len(pieces), largest / len(pieces)))
        factor_of = factor_of * jnp.repeat(heights, dims[dim] // blocks).reshape([-1 if axis == dim else 1 for axis in range(len(dims))])
    return factor_of


def length_profile(number_of, total, reach, lean):
    loads = [(1 << 20) // math.isqrt(standing ** lean) + 1 for standing in range(2, number_of + 1)]
    spare, counts = total - reach - (number_of - 1), [1] * (number_of - 1)
    while spare > 0:
        candidates = [i for i in range(number_of - 1) if counts[i] < reach]
        whole, budget = sum([loads[i] for i in candidates]), spare
        for i in candidates:
            more = min(reach - counts[i], max(1, budget * loads[i] // whole), spare)
            counts[i] = counts[i] + more
            spare = spare - more
    return np.array([reach] + counts)


def uneven_parts(key, amount, total, most, slope):
    if amount == 2:
        one = jax.random.randint(key, (), max(1, total - most), min(most, total - 1) + 1)
        return jnp.stack([one, total - one])
    tallies = jnp.asarray(length_profile(amount, total, most, slope), jnp.int32)
    pairs = (amount - 1) // 2
    donor, taker = tallies[1:1 + 2 * pairs:2], tallies[2:2 + 2 * pairs:2]
    room = jnp.minimum(donor - 1, most - taker)
    shifted = jax.random.randint(jax.random.fold_in(key, 1), (pairs,), 0, 1 << 20) % (room + 1)
    tallies = tallies.at[1:1 + 2 * pairs:2].set(donor - shifted).at[2:2 + 2 * pairs:2].set(taker + shifted)
    return tallies[jax.random.permutation(jax.random.fold_in(key, 2), amount)]


def bell_draw(stream_key, dims, spread, most, split=(), kind=jnp.bfloat16):
    array = spread * jax.random.normal(stream_key, dims, jnp.float32)
    if split:
        array = array * block_levels(stream_key, dims, split, -0.22, 0.18)
    return jnp.clip(array, -most, most).astype(kind)


def setup_inputs(seed: int = 0) -> dict:
    key_of = jax.random.split(jax.random.key(seed), 7)
    queries = draw_queries(jax.random.fold_in(key_of[6], 71), 0)
    keys = draw_keys(jax.random.fold_in(key_of[6], 71), 0)
    values = bell_draw(key_of[2], (PACKED_ROWS, SEQ_LEN, HEAD_DIM), 1.0, 6.0, ((1, 4),))
    d_out = bell_draw(key_of[3], (ROW_HEADS, SEQ_LEN, HEAD_DIM), 2.0, 12.0, ((0, 8), (1, 4)))
    doc_lengths = jax.vmap(lambda own: uneven_parts(own, DOC_COUNT, SEQ_LEN, DOC_MOST, 2))(jax.random.split(key_of[4], PACKED_ROWS)).reshape((PACKED_ROWS, DOC_COUNT)).astype(jnp.int32)
    fold_order = jax.random.permutation(key_of[5], BLOCK_COUNT).astype(jnp.int32)
    return {"queries": queries, "keys": keys, "values": values, "d_out": d_out, "doc_lengths": doc_lengths, "fold_order": fold_order}


masked_value = -1e30


def reference(queries, keys, values, d_out, doc_lengths, fold_order):
    scaling = HEAD_DIM ** -0.5
    indices = jnp.arange(SEQ_LEN, dtype=jnp.int32)
    position = fold_order[indices // BLOCK_LEN] * BLOCK_LEN + indices % BLOCK_LEN
    query_grads = []
    key_grads = []
    value_grads = []
    for row_index in range(PACKED_ROWS):
        lengths = doc_lengths[row_index]
        starts = jnp.cumsum(lengths, dtype=jnp.int32) - lengths
        document = jnp.sum((position[:, None] >= starts[None, :]).astype(jnp.int32), axis=1, dtype=jnp.int32)
        allowed = (document[:, None] == document[None, :]) & (position[None, :] <= position[:, None])
        key_row = keys[row_index]
        value_row = values[row_index]
        key_total = jnp.zeros((SEQ_LEN, HEAD_DIM), jnp.float32)
        value_total = jnp.zeros((SEQ_LEN, HEAD_DIM), jnp.float32)
        for head_index in range(HEAD_COUNT):
            pair_index = row_index * HEAD_COUNT + head_index
            query_rows = queries[pair_index]
            grad_out = d_out[pair_index]
            scores = jnp.where(allowed, jnp.dot(query_rows, key_row.T, preferred_element_type=jnp.float32) * scaling, masked_value)
            row_max = jnp.max(scores, axis=1, keepdims=True)
            log_norm = row_max + jnp.log(jnp.sum(jnp.exp(scores - row_max), axis=1, keepdims=True))
            weights = jnp.exp(scores - log_norm)
            weights_low = weights.astype(jnp.bfloat16)
            output = jnp.dot(weights_low, value_row, preferred_element_type=jnp.float32)
            grad_dot = jnp.sum(grad_out.astype(jnp.float32) * output, axis=1, keepdims=True)
            grad_prob = jnp.dot(grad_out, value_row.T, preferred_element_type=jnp.float32)
            grad_score = (weights * (grad_prob - grad_dot)).astype(jnp.bfloat16)
            query_grads.append((jnp.dot(grad_score, key_row, preferred_element_type=jnp.float32) * scaling).astype(jnp.bfloat16))
            key_total = key_total + jnp.dot(grad_score.T, query_rows, preferred_element_type=jnp.float32) * scaling
            value_total = value_total + jnp.dot(weights_low.T, grad_out, preferred_element_type=jnp.float32)
        key_grads.append(key_total)
        value_grads.append(value_total)
    return jnp.stack(query_grads), jnp.stack(key_grads), jnp.stack(value_grads)
```

```python
import functools
import math

import jax
import jax.numpy as jnp
from jax import lax
from jax.experimental import pallas as pl
from jax.experimental.pallas import tpu as pltpu
from jax.sharding import PartitionSpec as P

HEAD_COUNT = 8
MASKED = -1e30
CORES = 2


def contract(left, right, left_dim, right_dim):
    return lax.dot_general(
        left, right, (((left_dim,), (right_dim,)), ((), ())), preferred_element_type=jnp.float32
    )


class Places:
    def __init__(self, docs_ref, fold_ref, local_len):
        seq_total = lax.axis_size("seq")
        self.fold_ref = fold_ref
        self.per_shard = fold_ref.shape[0] // seq_total
        self.block = local_len // self.per_shard
        row = lax.axis_index("head") // HEAD_COUNT
        starts = [jnp.int32(0)]
        for d in range(docs_ref.shape[1] - 1):
            starts.append(starts[-1] + docs_ref[row, d])
        self.starts = starts

    def base(self, shard, index):
        return self.fold_ref[shard * self.per_shard + index] * self.block

    def row_place(self, base):
        position = base + lax.broadcasted_iota(jnp.int32, (1, self.block), 1)
        start = jnp.zeros((1, self.block), jnp.int32)
        first = jnp.int32(0)
        for d in self.starts[1:]:
            start = jnp.where(position >= d, d, start)
            first = jnp.where(base >= d, d, first)
        return position, start, first

    def active(self, query_base, first, key_base):
        return (key_base <= query_base) & (key_base + self.block > first)

    def allowed(self, query_place, key_base):
        position, start, _ = query_place
        key_position = key_base + lax.broadcasted_iota(jnp.int32, (self.block, self.block), 0)
        return (key_position >= start) & (key_position <= position)


def masked_scores(keys, query, allowed, factor):
    return jnp.where(allowed, contract(keys, query, 1, 1) * factor, MASKED)


def shard_at(offset):
    total = lax.axis_size("seq")
    return lax.rem(lax.axis_index("seq") + offset * CORES, total)


def stats_body(offset, factor, docs, fold, query, grad, key_own, value_own, key_sib, value_sib, out):
    place = Places(docs, fold, query.shape[0])
    block = place.block
    own = lax.axis_index("seq")
    query_shard = shard_at(offset)
    for i in range(place.per_shard):
        rows = pl.ds(i * block, block)
        base = place.base(query_shard, i)
        query_place = place.row_place(base)
        out[0:1, rows] = jnp.full((1, block), MASKED, jnp.float32)
        out[1:3, rows] = jnp.zeros((2, block), jnp.float32)
        for shard, keys, values in ((own, key_own, value_own), (own ^ 1, key_sib, value_sib)):
            for j in range(place.per_shard):
                key_base = place.base(shard, j)
                cols = pl.ds(j * block, block)

                @pl.when(place.active(base, query_place[2], key_base))
                def _():
                    scores = masked_scores(
                        keys[cols, :], query[rows, :], place.allowed(query_place, key_base), factor
                    )
                    prob = contract(values[cols, :], grad[rows, :], 1, 1)
                    old_max = out[0:1, rows]
                    new_max = jnp.maximum(old_max, jnp.max(scores, axis=0, keepdims=True))
                    keep = jnp.exp2(old_max - new_max)
                    weights = jnp.exp2(scores - new_max)
                    out[0:1, rows] = new_max
                    out[1:2, rows] = out[1:2, rows] * keep + jnp.sum(weights, axis=0, keepdims=True)
                    out[2:3, rows] = out[2:3, rows] * keep + jnp.sum(
                        weights * prob, axis=0, keepdims=True
                    )


def grads_body(offset, factor, parts, first, last, *refs):
    docs, fold, query, grad, key_own, value_own, key_sib, value_sib = refs[:8]
    stats = refs[8 : 8 + parts]
    rest = list(refs[8 + parts :])
    prior = None if first else (rest.pop(0), rest.pop(0))
    dq = rest.pop(0)
    outs = [rest.pop(0) for _ in range(4 if last else 2)]
    acc_key, acc_value, acc_query = rest
    place = Places(docs, fold, query.shape[0])
    block = place.block
    own = lax.axis_index("seq")
    query_shard = shard_at(offset)
    local = query.shape[0]
    if first:
        acc_key[...] = jnp.zeros_like(acc_key)
        acc_value[...] = jnp.zeros_like(acc_value)
    else:
        acc_key[...] = prior[0][...]
        acc_value[...] = prior[1][...]
    acc_query[...] = jnp.zeros_like(acc_query)
    top = stats[0][0:1, :]
    for part in stats[1:]:
        top = jnp.maximum(top, part[0:1, :])
    total = jnp.zeros_like(top)
    dots = jnp.zeros_like(top)
    for part in stats:
        keep = jnp.exp2(part[0:1, :] - top)
        total = total + part[1:2, :] * keep
        dots = dots + part[2:3, :] * keep
    norm = top + jnp.log2(total)
    dots = dots / total
    for i in range(place.per_shard):
        rows = pl.ds(i * block, block)
        base = place.base(query_shard, i)
        query_place = place.row_place(base)
        norm_i = norm[:, i * block : (i + 1) * block]
        dots_i = dots[:, i * block : (i + 1) * block]
        for side, (shard, keys, values) in enumerate(
            ((own, key_own, value_own), (own ^ 1, key_sib, value_sib))
        ):
            for j in range(place.per_shard):
                key_base = place.base(shard, j)
                cols = pl.ds(j * block, block)
                accs = pl.ds(side * local + j * block, block)

                @pl.when(place.active(base, query_place[2], key_base))
                def _():
                    q, g, k = query[rows, :], grad[rows, :], keys[cols, :]
                    scores = masked_scores(k, q, place.allowed(query_place, key_base), factor)
                    weights = jnp.exp2(scores - norm_i)
                    prob = contract(values[cols, :], g, 1, 1)
                    slope = (weights * (prob - dots_i)).astype(jnp.bfloat16)
                    acc_value[accs, :] += contract(weights.astype(jnp.bfloat16), g, 1, 0)
                    acc_key[accs, :] += contract(slope, q, 1, 0)
                    acc_query[rows, :] += contract(slope, k, 0, 0)

    dq[...] = acc_query[...].astype(dq.dtype)
    if last:
        for acc, mine, other in ((acc_key, outs[0], outs[2]), (acc_value, outs[1], outs[3])):
            mine[...] = acc[0:local, :]
            other[...] = acc[local : 2 * local, :].astype(other.dtype)
    else:
        outs[0][...] = acc_key[...]
        outs[1][...] = acc_value[...]


def pieces_body(scaling, dk, dv, dk_in, dv_in, mine, *outs):
    heads = lax.axis_size("head")
    head = lax.axis_index("head")
    piece = mine.shape[1]
    for step in range(heads):
        target = lax.rem(head + step, heads)
        rows = pl.ds(pl.multiple_of(target * piece, piece), piece)
        key_sum = (dk[rows, :] + dk_in[rows, :].astype(jnp.float32)) * scaling
        value_sum = dv[rows, :] + dv_in[rows, :].astype(jnp.float32)
        out = mine if step == 0 else outs[step - 1]
        out[0] = key_sum.astype(out.dtype)
        out[1] = value_sum.astype(out.dtype)


SMEM = pl.BlockSpec(memory_space=pltpu.SMEM)
VMEM = pl.BlockSpec(memory_space=pltpu.VMEM)


def shift(x, axis, amount):
    size = lax.axis_size(axis)
    return lax.ppermute(x, axis, [(i, (i - amount) % size) for i in range(size)])


def swap_cores(x):
    return lax.ppermute(x, "seq", [(i, i ^ 1) for i in range(lax.axis_size("seq"))])


def per_device(queries, keys, values, d_out, doc_lengths, fold_order):
    local, width = queries.shape[1:]
    chips = lax.axis_size("seq") // CORES
    heads = lax.axis_size("head")
    row_count = keys.shape[0]
    piece = local // heads
    scaling = width ** (-0.5)
    factor = scaling * math.log2(math.e)
    row_index = lax.axis_index("head") // HEAD_COUNT
    if row_count == 1:
        key_own, value_own = keys[0], values[0]
    else:
        key_own = lax.dynamic_index_in_dim(keys, row_index, 0, keepdims=False)
        value_own = lax.dynamic_index_in_dim(values, row_index, 0, keepdims=False)
    sets = [(queries[0], d_out[0])]
    for offset in range(1, chips):
        sets.append(
            (shift(queries[0], "seq", offset * CORES), shift(d_out[0], "seq", offset * CORES))
        )
    key_sib, value_sib = swap_cores(key_own), swap_cores(value_own)
    chip_keys = (key_own, value_own, key_sib, value_sib)
    tiles = local * 2 * local * width

    stats = []
    for offset in range(chips):
        stats.append(
            pl.pallas_call(
                functools.partial(stats_body, offset, factor),
                out_shape=jax.ShapeDtypeStruct((3, local), jnp.float32),
                in_specs=[SMEM] * 2 + [VMEM] * 6,
                out_specs=VMEM,
                name=f"stats{offset}",
                cost_estimate=pl.CostEstimate(
                    flops=4 * tiles, bytes_accessed=6 * local * width * 2, transcendentals=0
                ),
            )(doc_lengths, fold_order, *sets[offset], *chip_keys)
        )
    far = {
        (step, offset): shift(stats[(offset - step) % chips], "seq", step * CORES)
        for step in range(1, chips)
        for offset in range(chips)
    }
    acc = None
    partial_queries = [None] * chips
    order = list(range(1, chips)) + [0]
    for n, offset in enumerate(order):
        first, last = n == 0, n == chips - 1
        parts = [stats[offset]] + [far[step, offset] for step in range(1, chips)]
        wide = jax.ShapeDtypeStruct((CORES * local, width), jnp.float32)
        mine = jax.ShapeDtypeStruct((local, width), jnp.float32)
        sent = jax.ShapeDtypeStruct((local, width), jnp.bfloat16)
        out_shape = [mine if offset == 0 else sent]
        out_shape += [mine, mine, sent, sent] if last else [wide, wide]
        operands = [doc_lengths, fold_order, *sets[offset], *chip_keys, *parts]
        operands += [] if first else list(acc)
        results = pl.pallas_call(
            functools.partial(grads_body, offset, factor, chips, first, last),
            out_shape=out_shape,
            in_specs=[SMEM] * 2 + [VMEM] * (len(operands) - 2),
            out_specs=[VMEM] * len(out_shape),
            scratch_shapes=[
                pltpu.VMEM((CORES * local, width), jnp.float32),
                pltpu.VMEM((CORES * local, width), jnp.float32),
                pltpu.VMEM((local, width), jnp.float32),
            ],
            name=f"grads{offset}",
            cost_estimate=pl.CostEstimate(
                flops=10 * tiles, bytes_accessed=8 * local * width * 4, transcendentals=0
            ),
        )(*operands)
        partial_queries[offset] = results[0]
        acc = results[1:]
    dk, dv, dk_out, dv_out = acc
    dk_in, dv_in = swap_cores(dk_out), swap_cores(dv_out)
    grad_query = partial_queries[0]
    for offset in range(1, chips):
        grad_query = grad_query + shift(
            partial_queries[offset], "seq", -offset * CORES
        ).astype(jnp.float32)
    grad_queries = (grad_query * scaling).astype(jnp.bfloat16)[None]

    moved = pl.pallas_call(
        functools.partial(pieces_body, scaling),
        out_shape=[jax.ShapeDtypeStruct((2, piece, width), jnp.float32)]
        + [jax.ShapeDtypeStruct((2, piece, width), jnp.bfloat16)] * (heads - 1),
        in_specs=[VMEM] * 4,
        out_specs=[VMEM] * heads,
        name="pieces",
        cost_estimate=pl.CostEstimate(
            flops=4 * local * width, bytes_accessed=8 * local * width * 4, transcendentals=0
        ),
    )(dk, dv, dk_in, dv_in)
    terms = [moved[0]]
    for step in range(1, heads):
        terms.append(shift(moved[step], "head", -step).astype(jnp.float32))
    head = lax.axis_index("head")
    rows = []
    for r in range(row_count):
        total = None
        for step, term in enumerate(terms):
            if row_count > 1:
                source = lax.rem(head - step + heads, heads) // HEAD_COUNT
                term = jnp.where(source == r, term, 0.0)
            total = term if total is None else total + term
        rows.append(total)
    grad_keys = jnp.stack([total[0] for total in rows])
    grad_values = jnp.stack([total[1] for total in rows])
    return grad_queries, grad_keys, grad_values


def solution(mesh):
    in_specs = (
        P("head", "seq", None),
        P(None, "seq", None),
        P(None, "seq", None),
        P("head", "seq", None),
        P(),
        P(),
    )
    out_specs = (
        P("head", "seq", None),
        P(None, ("seq", "head"), None),
        P(None, ("seq", "head"), None),
    )
    return jax.shard_map(
        per_device, mesh=mesh, in_specs=in_specs, out_specs=out_specs, check_vma=False
    )
```

```python
import functools
import math

import jax
import jax.numpy as jnp
from jax import lax
from jax.experimental import pallas as pl
from jax.experimental.pallas import tpu as pltpu
from jax.sharding import PartitionSpec as P

HEAD_COUNT = 8
MASKED = -1e30
VMEM_LIMIT = 14 * 1024 * 1024
CORES = 2


def contract(left, right, left_dim, right_dim):
    return lax.dot_general(
        left, right, (((left_dim,), (right_dim,)), ((), ())), preferred_element_type=jnp.float32
    )


class Places:
    def __init__(self, docs_ref, fold_ref, local_len):
        seq_total = lax.axis_size("seq")
        self.fold_ref = fold_ref
        self.per_shard = fold_ref.shape[0] // seq_total
        self.block = local_len // self.per_shard
        row = lax.axis_index("head") // HEAD_COUNT
        starts = [jnp.int32(0)]
        for d in range(docs_ref.shape[1] - 1):
            starts.append(starts[-1] + docs_ref[row, d])
        self.starts = starts

    def base(self, shard, index):
        return self.fold_ref[shard * self.per_shard + index] * self.block

    def row_place(self, base):
        position = base + lax.broadcasted_iota(jnp.int32, (1, self.block), 1)
        start = jnp.zeros((1, self.block), jnp.int32)
        first = jnp.int32(0)
        for d in self.starts[1:]:
            start = jnp.where(position >= d, d, start)
            first = jnp.where(base >= d, d, first)
        return position, start, first

    def active(self, query_base, first, key_base):
        return (key_base <= query_base) & (key_base + self.block > first)

    def allowed(self, query_place, key_base):
        position, start, _ = query_place
        key_position = key_base + lax.broadcasted_iota(jnp.int32, (self.block, self.block), 0)
        return (key_position >= start) & (key_position <= position)


def masked_scores(keys, query, allowed, factor):
    return jnp.where(allowed, contract(keys, query, 1, 1) * factor, MASKED)


def shard_at(offset):
    total = lax.axis_size("seq")
    return lax.rem(lax.axis_index("seq") + offset * CORES, total)


def stats_body(offset, factor, docs, fold, query, grad, key_own, value_own, key_sib, value_sib, out):
    place = Places(docs, fold, query.shape[0])
    block = place.block
    own = lax.axis_index("seq")
    query_shard = shard_at(offset)
    for i in range(place.per_shard):
        rows = pl.ds(i * block, block)
        base = place.base(query_shard, i)
        query_place = place.row_place(base)
        out[0:1, rows] = jnp.full((1, block), MASKED, jnp.float32)
        out[1:3, rows] = jnp.zeros((2, block), jnp.float32)
        for shard, keys, values in ((own, key_own, value_own), (own ^ 1, key_sib, value_sib)):
            for j in range(place.per_shard):
                key_base = place.base(shard, j)
                cols = pl.ds(j * block, block)

                @pl.when(place.active(base, query_place[2], key_base))
                def _():
                    scores = masked_scores(
                        keys[cols, :], query[rows, :], place.allowed(query_place, key_base), factor
                    )
                    prob = contract(values[cols, :], grad[rows, :], 1, 1)
                    old_max = out[0:1, rows]
                    new_max = jnp.maximum(old_max, jnp.max(scores, axis=0, keepdims=True))
                    keep = jnp.exp2(old_max - new_max)
                    weights = jnp.exp2(scores - new_max)
                    out[0:1, rows] = new_max
                    out[1:2, rows] = out[1:2, rows] * keep + jnp.sum(weights, axis=0, keepdims=True)
                    out[2:3, rows] = out[2:3, rows] * keep + jnp.sum(
                        weights * prob, axis=0, keepdims=True
                    )


def grads_body(offset, factor, parts, first, last, *refs):
    docs, fold, query, grad, key_own, value_own, key_sib, value_sib = refs[:8]
    stats = refs[8 : 8 + parts]
    rest = list(refs[8 + parts :])
    prior = None if first else (rest.pop(0), rest.pop(0))
    dq = rest.pop(0)
    outs = [rest.pop(0) for _ in range(4 if last else 2)]
    acc_key, acc_value, acc_query = rest
    place = Places(docs, fold, query.shape[0])
    block = place.block
    own = lax.axis_index("seq")
    query_shard = shard_at(offset)
    local = query.shape[0]
    if first:
        acc_key[...] = jnp.zeros_like(acc_key)
        acc_value[...] = jnp.zeros_like(acc_value)
    else:
        acc_key[...] = prior[0][...]
        acc_value[...] = prior[1][...]
    acc_query[...] = jnp.zeros_like(acc_query)
    top = stats[0][0:1, :]
    for part in stats[1:]:
        top = jnp.maximum(top, part[0:1, :])
    total = jnp.zeros_like(top)
    dots = jnp.zeros_like(top)
    for part in stats:
        keep = jnp.exp2(part[0:1, :] - top)
        total = total + part[1:2, :] * keep
        dots = dots + part[2:3, :] * keep
    norm = top + jnp.log2(total)
    dots = dots / total
    for i in range(place.per_shard):
        rows = pl.ds(i * block, block)
        base = place.base(query_shard, i)
        query_place = place.row_place(base)
        norm_i = norm[:, i * block : (i + 1) * block]
        dots_i = dots[:, i * block : (i + 1) * block]
        for side, (shard, keys, values) in enumerate(
            ((own, key_own, value_own), (own ^ 1, key_sib, value_sib))
        ):
            for j in range(place.per_shard):
                key_base = place.base(shard, j)
                cols = pl.ds(j * block, block)
                accs = pl.ds(side * local + j * block, block)

                @pl.when(place.active(base, query_place[2], key_base))
                def _():
                    q, g, k = query[rows, :], grad[rows, :], keys[cols, :]
                    scores = masked_scores(k, q, place.allowed(query_place, key_base), factor)
                    weights = jnp.exp2(scores - norm_i)
                    prob = contract(values[cols, :], g, 1, 1)
                    slope = (weights * (prob - dots_i)).astype(jnp.bfloat16)
                    acc_value[accs, :] += contract(weights.astype(jnp.bfloat16), g, 1, 0)
                    acc_key[accs, :] += contract(slope, q, 1, 0)
                    acc_query[rows, :] += contract(slope, k, 0, 0)

    dq[...] = acc_query[...].astype(dq.dtype)
    if last:
        for acc, mine, other in ((acc_key, outs[0], outs[2]), (acc_value, outs[1], outs[3])):
            mine[...] = acc[0:local, :]
            other[...] = acc[local : 2 * local, :].astype(other.dtype)
    else:
        outs[0][...] = acc_key[...]
        outs[1][...] = acc_value[...]


def pieces_body(scaling, dk, dv, dk_in, dv_in, mine, *outs):
    heads = lax.axis_size("head")
    head = lax.axis_index("head")
    piece = mine.shape[1]
    for step in range(heads):
        target = lax.rem(head + step, heads)
        rows = pl.ds(pl.multiple_of(target * piece, piece), piece)
        key_sum = (dk[rows, :] + dk_in[rows, :].astype(jnp.float32)) * scaling
        value_sum = dv[rows, :] + dv_in[rows, :].astype(jnp.float32)
        out = mine if step == 0 else outs[step - 1]
        out[0] = key_sum.astype(out.dtype)
        out[1] = value_sum.astype(out.dtype)


SMEM = pl.BlockSpec(memory_space=pltpu.SMEM)
VMEM = pl.BlockSpec(memory_space=pltpu.VMEM)


def shift(x, axis, amount):
    size = lax.axis_size(axis)
    return lax.ppermute(x, axis, [(i, (i - amount) % size) for i in range(size)])


def swap_cores(x):
    return lax.ppermute(x, "seq", [(i, i ^ 1) for i in range(lax.axis_size("seq"))])


def per_device(queries, keys, values, d_out, doc_lengths, fold_order):
    local, width = queries.shape[1:]
    chips = lax.axis_size("seq") // CORES
    heads = lax.axis_size("head")
    row_count = keys.shape[0]
    piece = local // heads
    scaling = width ** (-0.5)
    factor = scaling * math.log2(math.e)
    row_index = lax.axis_index("head") // HEAD_COUNT
    if row_count == 1:
        key_own, value_own = keys[0], values[0]
    else:
        key_own = lax.dynamic_index_in_dim(keys, row_index, 0, keepdims=False)
        value_own = lax.dynamic_index_in_dim(values, row_index, 0, keepdims=False)
    sets = [(queries[0], d_out[0])]
    for offset in range(1, chips):
        sets.append(
            (shift(queries[0], "seq", offset * CORES), shift(d_out[0], "seq", offset * CORES))
        )
    key_sib, value_sib = swap_cores(key_own), swap_cores(value_own)
    chip_keys = (key_own, value_own, key_sib, value_sib)
    tiles = local * 2 * local * width

    stats = []
    for offset in range(chips):
        stats.append(
            pl.pallas_call(
                functools.partial(stats_body, offset, factor),
                out_shape=jax.ShapeDtypeStruct((3, local), jnp.float32),
                in_specs=[SMEM] * 2 + [VMEM] * 6,
                out_specs=VMEM,
                name=f"stats{offset}",
                compiler_params=pltpu.CompilerParams(vmem_limit_bytes=VMEM_LIMIT),
                cost_estimate=pl.CostEstimate(
                    flops=4 * tiles, bytes_accessed=6 * local * width * 2, transcendentals=0
                ),
            )(doc_lengths, fold_order, *sets[offset], *chip_keys)
        )
    far = {
        (step, offset): shift(stats[(offset - step) % chips], "seq", step * CORES)
        for step in range(1, chips)
        for offset in range(chips)
    }
    acc = None
    partial_queries = [None] * chips
    order = list(range(1, chips)) + [0]
    for n, offset in enumerate(order):
        first, last = n == 0, n == chips - 1
        parts = [stats[offset]] + [far[step, offset] for step in range(1, chips)]
        wide = jax.ShapeDtypeStruct((CORES * local, width), jnp.float32)
        mine = jax.ShapeDtypeStruct((local, width), jnp.float32)
        sent = jax.ShapeDtypeStruct((local, width), jnp.bfloat16)
        out_shape = [mine if offset == 0 else sent]
        out_shape += [mine, mine, sent, sent] if last else [wide, wide]
        operands = [doc_lengths, fold_order, *sets[offset], *chip_keys, *parts]
        operands += [] if first else list(acc)
        results = pl.pallas_call(
            functools.partial(grads_body, offset, factor, chips, first, last),
            out_shape=out_shape,
            in_specs=[SMEM] * 2 + [VMEM] * (len(operands) - 2),
            out_specs=[VMEM] * len(out_shape),
            scratch_shapes=[
                pltpu.VMEM((CORES * local, width), jnp.float32),
                pltpu.VMEM((CORES * local, width), jnp.float32),
                pltpu.VMEM((local, width), jnp.float32),
            ],
            name=f"grads{offset}",
            compiler_params=pltpu.CompilerParams(vmem_limit_bytes=VMEM_LIMIT),
                cost_estimate=pl.CostEstimate(
                flops=10 * tiles, bytes_accessed=8 * local * width * 4, transcendentals=0
            ),
        )(*operands)
        partial_queries[offset] = results[0]
        acc = results[1:]
    dk, dv, dk_out, dv_out = acc
    dk_in, dv_in = swap_cores(dk_out), swap_cores(dv_out)
    grad_query = partial_queries[0]
    for offset in range(1, chips):
        grad_query = grad_query + shift(
            partial_queries[offset], "seq", -offset * CORES
        ).astype(jnp.float32)
    grad_queries = (grad_query * scaling).astype(jnp.bfloat16)[None]

    moved = pl.pallas_call(
        functools.partial(pieces_body, scaling),
        out_shape=[jax.ShapeDtypeStruct((2, piece, width), jnp.float32)]
        + [jax.ShapeDtypeStruct((2, piece, width), jnp.bfloat16)] * (heads - 1),
        in_specs=[VMEM] * 4,
        out_specs=[VMEM] * heads,
        name="pieces",
        compiler_params=pltpu.CompilerParams(vmem_limit_bytes=VMEM_LIMIT),
                cost_estimate=pl.CostEstimate(
            flops=4 * local * width, bytes_accessed=8 * local * width * 4, transcendentals=0
        ),
    )(dk, dv, dk_in, dv_in)
    terms = [moved[0]]
    for step in range(1, heads):
        terms.append(shift(moved[step], "head", -step).astype(jnp.float32))
    head = lax.axis_index("head")
    rows = []
    for r in range(row_count):
        total = None
        for step, term in enumerate(terms):
            if row_count > 1:
                source = lax.rem(head - step + heads, heads) // HEAD_COUNT
                term = jnp.where(source == r, term, 0.0)
            total = term if total is None else total + term
        rows.append(total)
    grad_keys = jnp.stack([total[0] for total in rows])
    grad_values = jnp.stack([total[1] for total in rows])
    return grad_queries, grad_keys, grad_values


def solution(mesh):
    in_specs = (
        P("head", "seq", None),
        P(None, "seq", None),
        P(None, "seq", None),
        P("head", "seq", None),
        P(),
        P(),
    )
    out_specs = (
        P("head", "seq", None),
        P(None, ("seq", "head"), None),
        P(None, ("seq", "head"), None),
    )
    return jax.shard_map(
        per_device, mesh=mesh, in_specs=in_specs, out_specs=out_specs, check_vma=False
    )
```

```python
import functools
import math

import jax
import jax.numpy as jnp
from jax import lax
from jax.experimental import pallas as pl
from jax.experimental.pallas import tpu as pltpu
from jax.sharding import PartitionSpec as P


HEAD_COUNT = 8
MASKED = -1e30
VMEM_LIMIT = 14 * 1024 * 1024
CORES = 2


def contract(left, right, left_dim, right_dim):
    return lax.dot_general(
        left, right, (((left_dim,), (right_dim,)), ((), ())), preferred_element_type=jnp.float32
    )


def place_body(local, docs, fold, *refs):
    for source, target in zip(refs[:4], refs[4:8]):
        target[...] = source[...]
    outs = refs[8:]
    seq_total = lax.axis_size("seq")
    per_shard = fold.shape[0] // seq_total
    block = local // per_shard
    own = lax.axis_index("seq")
    row = lax.axis_index("head") // HEAD_COUNT
    starts = [jnp.int32(0)]
    for d in range(docs.shape[1] - 1):
        starts.append(starts[-1] + docs[row, d])
    key_bases = [
        fold[shard * per_shard + j] * block for shard in (own, own ^ 1) for j in range(per_shard)
    ]
    for offset in range(len(outs) // 2):
        info, word = outs[2 * offset : 2 * offset + 2]
        shard = lax.rem(own + offset * CORES, seq_total)
        bits = jnp.int32(0)
        for i in range(per_shard):
            base = fold[shard * per_shard + i] * block
            position = base + lax.broadcasted_iota(jnp.int32, (1, block), 1)
            start = jnp.zeros((1, block), jnp.int32)
            first = jnp.int32(0)
            for d in starts[1:]:
                start = jnp.where(position >= d, d, start)
                first = jnp.where(base >= d, d, first)
            for j, key_base in enumerate(key_bases):
                tile = i * len(key_bases) + j
                info[2 * tile : 2 * tile + 1, :] = start - key_base
                info[2 * tile + 1 : 2 * tile + 2, :] = position - key_base
                active = (key_base <= base) & (key_base + block > first)
                bits = bits | jnp.where(active, 1 << tile, 0)
        word[...] = jnp.full(word.shape, bits, jnp.int32)


def tile_bit(bits, tile):
    return ((bits >> tile) & 1) == 1


def stats_body(factor, info, word, query, grad, *refs):
    keys, values = refs[0:2], refs[2:4]
    out, scores_out, prob_out = refs[4:]
    local = query.shape[0]
    block = info.shape[1]
    per_shard = local // block
    bits = jnp.max(word[...])
    key_index = lax.broadcasted_iota(jnp.int32, (block, block), 0)
    for i in range(per_shard):
        rows = pl.ds(i * block, block)
        out[0:1, rows] = jnp.full((1, block), MASKED, jnp.float32)
        out[1:3, rows] = jnp.zeros((2, block), jnp.float32)
        for j in range(CORES * per_shard):
            tile = i * CORES * per_shard + j
            side, cols = j // per_shard, pl.ds(j % per_shard * block, block)
            held = pl.ds(j * block, block)

            @pl.when(tile_bit(bits, tile))
            def _():
                allowed = (key_index >= info[2 * tile : 2 * tile + 1, :]) & (
                    key_index <= info[2 * tile + 1 : 2 * tile + 2, :]
                )
                scores = contract(keys[side][cols, :], query[rows, :], 1, 1) * factor
                scores = jnp.where(allowed, scores, MASKED)
                prob = contract(values[side][cols, :], grad[rows, :], 1, 1)
                scores_out[held, rows] = scores
                prob_out[held, rows] = prob
                old_max = out[0:1, rows]
                new_max = jnp.maximum(old_max, jnp.max(scores, axis=0, keepdims=True))
                keep = jnp.exp2(old_max - new_max)
                weights = jnp.exp2(scores - new_max)
                out[0:1, rows] = new_max
                out[1:2, rows] = out[1:2, rows] * keep + jnp.sum(weights, axis=0, keepdims=True)
                out[2:3, rows] = out[2:3, rows] * keep + jnp.sum(
                    weights * prob, axis=0, keepdims=True
                )


def grads_body(parts, first, last, word, scores, probs, query, grad, *refs):
    keys = refs[0:2]
    stats = refs[2 : 2 + parts]
    rest = list(refs[2 + parts :])
    prior = None if first else (rest.pop(0), rest.pop(0))
    dq = rest.pop(0)
    outs = [rest.pop(0) for _ in range(4 if last else 2)]
    acc_key, acc_value, acc_query = rest
    local = query.shape[0]
    block = acc_query.shape[0]
    per_shard = local // block
    tiles = CORES * per_shard
    bits = jnp.max(word[...])
    top = stats[0][0:1, :]
    for part in stats[1:]:
        top = jnp.maximum(top, part[0:1, :])
    total = jnp.zeros_like(top)
    dots = jnp.zeros_like(top)
    for part in stats:
        keep = jnp.exp2(part[0:1, :] - top)
        total = total + part[1:2, :] * keep
        dots = dots + part[2:3, :] * keep
    norm = top + jnp.log2(total)
    dots = dots / total

    def settle(active, target, source, term):
        ref, at = target
        if active:
            value = term()
            if source is not None:
                value = value + source[0][source[1], :]
            ref[at, :] = value.astype(ref.dtype)
        elif source is None:
            ref[at, :] = jnp.zeros((block, ref.shape[1]), ref.dtype)
        elif source[0] is not ref:
            ref[at, :] = source[0][source[1], :].astype(ref.dtype)

    for i in range(per_shard):
        rows = pl.ds(i * block, block)
        norm_i = norm[:, i * block : (i + 1) * block]
        dots_i = dots[:, i * block : (i + 1) * block]
        for j in range(tiles):
            side, cols = j // per_shard, pl.ds(j % per_shard * block, block)
            held = pl.ds(j * block, block)
            query_source = None if j == 0 else (acc_query, pl.ds(0, block))
            query_target = (dq, rows) if j == tiles - 1 else (acc_query, pl.ds(0, block))
            sources = []
            targets = []
            for n, acc in enumerate((acc_key, acc_value)):
                if i > 0:
                    sources.append((acc, held))
                else:
                    sources.append(None if first else (prior[n], held))
                if i < per_shard - 1:
                    targets.append((acc, held))
                elif last:
                    targets.append((outs[n + 2 * side], cols))
                else:
                    targets.append((outs[n], held))
            bit = tile_bit(bits, i * tiles + j)

            @pl.when(bit)
            def _():
                g, q = grad[rows, :], query[rows, :]
                weights = jnp.exp2(scores[held, rows] - norm_i)
                slope = (weights * (probs[held, rows] - dots_i)).astype(jnp.bfloat16)
                settle(
                    True,
                    targets[1],
                    sources[1],
                    lambda: contract(weights.astype(jnp.bfloat16), g, 1, 0),
                )
                settle(True, targets[0], sources[0], lambda: contract(slope, q, 1, 0))
                settle(
                    True,
                    query_target,
                    query_source,
                    lambda: contract(slope, keys[side][cols, :], 0, 0),
                )

            @pl.when(jnp.logical_not(bit))
            def _():
                settle(False, targets[1], sources[1], None)
                settle(False, targets[0], sources[0], None)
                settle(False, query_target, query_source, None)


def split_body(scaling, order, dk, dv, dk_in, dv_in, *outs):
    head = lax.axis_index("head")
    piece = outs[0].shape[1]
    for step, out in zip([0] + order, outs):
        rows = pl.ds(pl.multiple_of(lax.rem(head + step, lax.axis_size("head")) * piece, piece), piece)
        key_sum = (dk[rows, :] + dk_in[rows, :].astype(jnp.float32)) * scaling
        value_sum = dv[rows, :] + dv_in[rows, :].astype(jnp.float32)
        out[0] = key_sum.astype(out.dtype)
        out[1] = value_sum.astype(out.dtype)


def exchange_order(heads):
    return list(range(1, heads))


def by_row(row_count, steps, terms):
    head = lax.axis_index("head")
    rows = []
    for r in range(row_count):
        total = None
        for step, term in zip(steps, terms):
            term = term.astype(jnp.float32)
            if row_count > 1:
                term = jnp.where(lax.rem(head - step + lax.axis_size("head"), lax.axis_size("head")) // HEAD_COUNT == r, term, 0.0)
            total = term if total is None else total + term
        rows.append(total)
    return rows


SMEM = pl.BlockSpec(memory_space=pltpu.SMEM)
VMEM = pl.BlockSpec(memory_space=pltpu.VMEM)


def shift(x, axis, amount):
    size = lax.axis_size(axis)
    return lax.ppermute(x, axis, [(i, (i - amount) % size) for i in range(size)])


def swap_cores(x):
    return lax.ppermute(x, "seq", [(i, i ^ 1) for i in range(lax.axis_size("seq"))])


def kernel(body, operands, outs, flops, scratch=()):
    return pl.pallas_call(
        body,
        out_shape=outs,
        in_specs=[SMEM if x.dtype == jnp.int32 and x.ndim < 2 else VMEM for x in operands],
        out_specs=[VMEM] * len(outs),
        scratch_shapes=list(scratch),
        compiler_params=pltpu.CompilerParams(vmem_limit_bytes=VMEM_LIMIT),
        cost_estimate=pl.CostEstimate(
            flops=int(flops), bytes_accessed=int(flops) // 256, transcendentals=0
        ),
    )(*operands)


def gradients(queries, keys, values, d_out, doc_lengths, fold_order):
    local, width = queries.shape[1:]
    chips = lax.axis_size("seq") // CORES
    heads = lax.axis_size("head")
    row_count = keys.shape[0]
    piece = local // heads
    block = local // (fold_order.shape[0] // lax.axis_size("seq"))
    tiles = (local // block) * (CORES * local // block)
    scaling = width ** (-0.5)
    factor = scaling * math.log2(math.e)
    row_index = lax.axis_index("head") // HEAD_COUNT
    full = jnp.float32
    low = jnp.bfloat16
    shape = jax.ShapeDtypeStruct

    sets = [(queries[0], d_out[0])]
    for offset in range(1, chips):
        sets.append(
            (shift(queries[0], "seq", offset * CORES), shift(d_out[0], "seq", offset * CORES))
        )
    if row_count == 1:
        key_own, value_own = keys[0], values[0]
    else:
        key_own = lax.dynamic_index_in_dim(keys, row_index, 0, keepdims=False)
        value_own = lax.dynamic_index_in_dim(values, row_index, 0, keepdims=False)
    key_sib, value_sib = swap_cores(key_own), swap_cores(value_own)
    own_arrays = (*sets[0], key_own, value_own)
    places = pl.pallas_call(
        functools.partial(place_body, local),
        out_shape=[shape((local, width), low)] * 4
        + [shape((2 * tiles, block), jnp.int32), shape((8, 128), jnp.int32)] * chips,
        in_specs=[SMEM] * 2 + [VMEM] * 4,
        out_specs=[VMEM] * (4 + 2 * chips),
        name="place",
        compiler_params=pltpu.CompilerParams(vmem_limit_bytes=VMEM_LIMIT),
        cost_estimate=pl.CostEstimate(flops=1 << 20, bytes_accessed=1 << 14, transcendentals=0),
    )(doc_lengths, fold_order, *own_arrays)
    sets[0] = tuple(places[:2])
    key_own, value_own = places[2:4]
    places = places[4:]

    work = 4 * local * CORES * local * width
    stats, held = [], []
    for offset in range(chips):
        info, word = places[2 * offset : 2 * offset + 2]
        pairs = shape((CORES * local, local), full)
        part, scores, probs = kernel(
            functools.partial(stats_body, factor),
            (info, word, *sets[offset], key_own, key_sib, value_own, value_sib),
            [shape((3, local), full), pairs, pairs],
            work,
        )
        stats.append(part)
        held.append((word, scores, probs))
    far = {
        (step, offset): shift(stats[(offset - step) % chips], "seq", step * CORES)
        for step in range(1, chips)
        for offset in range(chips)
    }
    acc = ()
    partial_queries = [None] * chips
    for n, offset in enumerate(list(range(1, chips)) + [0]):
        first, last = n == 0, n == chips - 1
        parts = [stats[offset]] + [far[step, offset] for step in range(1, chips)]
        mine, sent = shape((local, width), full), shape((local, width), low)
        wide = shape((CORES * local, width), full)
        results = kernel(
            functools.partial(grads_body, chips, first, last),
            (*held[offset], *sets[offset], key_own, key_sib, *parts, *acc),
            [mine if offset == 0 else sent] + ([mine, mine, sent, sent] if last else [wide, wide]),
            1.5 * work,
            [pltpu.VMEM((CORES * local, width), full)] * 2 + [pltpu.VMEM((block, width), full)],
        )
        partial_queries[offset] = results[0]
        acc = results[1:]
    dk, dv, dk_out, dv_out = acc
    dk_in, dv_in = swap_cores(dk_out), swap_cores(dv_out)
    grad_query = partial_queries[0]
    for offset in range(1, chips):
        grad_query = grad_query + shift(
            partial_queries[offset], "seq", -offset * CORES
        ).astype(full)
    grad_queries = (grad_query * scaling).astype(low)[None]

    order = exchange_order(heads)
    moved = kernel(
        functools.partial(split_body, scaling, order),
        (dk, dv, dk_in, dv_in),
        [shape((2, piece, width), full)] + [shape((2, piece, width), low)] * (heads - 1),
        4 * local * width,
    )
    terms = [moved[0]]
    for step, x in zip(order, moved[1:]):
        terms.append(shift(x, "head", -step))
    rows = by_row(row_count, [0] + order, terms)
    grad_keys = jnp.stack([total[0] for total in rows])
    grad_values = jnp.stack([total[1] for total in rows])
    return grad_queries, grad_keys, grad_values


def solution(mesh):
    in_specs = (
        P("head", "seq", None),
        P(None, "seq", None),
        P(None, "seq", None),
        P("head", "seq", None),
        P(),
        P(),
    )
    out_specs = (
        P("head", "seq", None),
        P(None, ("seq", "head"), None),
        P(None, ("seq", "head"), None),
    )
    return jax.shard_map(
        gradients, mesh=mesh, in_specs=in_specs, out_specs=out_specs, check_vma=False
    )
```

```python
import functools
import math

import jax
import jax.numpy as jnp
from jax import lax
from jax.experimental import pallas as pl
from jax.experimental.pallas import tpu as pltpu
from jax.sharding import PartitionSpec as P


HEAD_COUNT = 8
MASKED = -1e30
VMEM_LIMIT = 14 * 1024 * 1024
CORES = 2
MINOR = 2


def contract(left, right, left_dim, right_dim):
    return lax.dot_general(
        left, right, (((left_dim,), (right_dim,)), ((), ())), preferred_element_type=jnp.float32
    )


def place_body(local, docs, fold, *refs):
    for source, target in zip(refs[:4], refs[4:8]):
        target[...] = source[...]
    outs = refs[8:]
    seq_total = lax.axis_size("seq")
    per_shard = fold.shape[0] // seq_total
    block = local // per_shard
    own = lax.axis_index("seq")
    row = lax.axis_index("head") // HEAD_COUNT
    starts = [jnp.int32(0)]
    for d in range(docs.shape[1] - 1):
        starts.append(starts[-1] + docs[row, d])
    key_bases = [
        fold[shard * per_shard + j] * block for shard in (own, own ^ 1) for j in range(per_shard)
    ]
    for offset in range(len(outs) // 2):
        info, word = outs[2 * offset : 2 * offset + 2]
        shard = lax.rem(own + offset * CORES, seq_total)
        bits = jnp.int32(0)
        for i in range(per_shard):
            base = fold[shard * per_shard + i] * block
            position = base + lax.broadcasted_iota(jnp.int32, (1, block), 1)
            start = jnp.zeros((1, block), jnp.int32)
            first = jnp.int32(0)
            for d in starts[1:]:
                start = jnp.where(position >= d, d, start)
                first = jnp.where(base >= d, d, first)
            for j, key_base in enumerate(key_bases):
                tile = i * len(key_bases) + j
                info[2 * tile : 2 * tile + 1, :] = start - key_base
                info[2 * tile + 1 : 2 * tile + 2, :] = position - key_base
                active = (key_base <= base) & (key_base + block > first)
                bits = bits | jnp.where(active, 1 << tile, 0)
        word[...] = jnp.full(word.shape, bits, jnp.int32)


def tile_bit(bits, tile):
    return ((bits >> tile) & 1) == 1


def stats_body(factor, info, word, query, grad, *refs):
    keys, values = refs[0:2], refs[2:4]
    out, scores_out, prob_out = refs[4:]
    local = query.shape[0]
    block = info.shape[1]
    per_shard = local // block
    bits = jnp.max(word[...])
    key_index = lax.broadcasted_iota(jnp.int32, (block, block), 0)
    for i in range(per_shard):
        rows = pl.ds(i * block, block)
        out[0:1, rows] = jnp.full((1, block), MASKED, jnp.float32)
        out[1:3, rows] = jnp.zeros((2, block), jnp.float32)
        for j in range(CORES * per_shard):
            tile = i * CORES * per_shard + j
            side, cols = j // per_shard, pl.ds(j % per_shard * block, block)
            held = pl.ds(j * block, block)

            @pl.when(tile_bit(bits, tile))
            def _():
                allowed = (key_index >= info[2 * tile : 2 * tile + 1, :]) & (
                    key_index <= info[2 * tile + 1 : 2 * tile + 2, :]
                )
                scores = contract(keys[side][cols, :], query[rows, :], 1, 1) * factor
                scores = jnp.where(allowed, scores, MASKED)
                prob = contract(values[side][cols, :], grad[rows, :], 1, 1)
                scores_out[held, rows] = scores
                prob_out[held, rows] = prob
                old_max = out[0:1, rows]
                new_max = jnp.maximum(old_max, jnp.max(scores, axis=0, keepdims=True))
                keep = jnp.exp2(old_max - new_max)
                weights = jnp.exp2(scores - new_max)
                out[0:1, rows] = new_max
                out[1:2, rows] = out[1:2, rows] * keep + jnp.sum(weights, axis=0, keepdims=True)
                out[2:3, rows] = out[2:3, rows] * keep + jnp.sum(
                    weights * prob, axis=0, keepdims=True
                )


def grads_body(parts, first, last, word, scores, probs, query, grad, *refs):
    keys = refs[0:2]
    stats = refs[2 : 2 + parts]
    rest = list(refs[2 + parts :])
    prior = None if first else (rest.pop(0), rest.pop(0))
    dq = rest.pop(0)
    outs = [rest.pop(0) for _ in range(4 if last else 2)]
    acc_key, acc_value, acc_query = rest
    local = query.shape[0]
    block = acc_query.shape[0]
    per_shard = local // block
    tiles = CORES * per_shard
    bits = jnp.max(word[...])
    top = stats[0][0:1, :]
    for part in stats[1:]:
        top = jnp.maximum(top, part[0:1, :])
    total = jnp.zeros_like(top)
    dots = jnp.zeros_like(top)
    for part in stats:
        keep = jnp.exp2(part[0:1, :] - top)
        total = total + part[1:2, :] * keep
        dots = dots + part[2:3, :] * keep
    norm = top + jnp.log2(total)
    dots = dots / total

    def settle(active, target, source, term):
        ref, at = target
        if active:
            value = term()
            if source is not None:
                value = value + source[0][source[1], :]
            ref[at, :] = value.astype(ref.dtype)
        elif source is None:
            ref[at, :] = jnp.zeros((block, ref.shape[1]), ref.dtype)
        elif source[0] is not ref:
            ref[at, :] = source[0][source[1], :].astype(ref.dtype)

    for i in range(per_shard):
        rows = pl.ds(i * block, block)
        norm_i = norm[:, i * block : (i + 1) * block]
        dots_i = dots[:, i * block : (i + 1) * block]
        for j in range(tiles):
            side, cols = j // per_shard, pl.ds(j % per_shard * block, block)
            held = pl.ds(j * block, block)
            query_source = None if j == 0 else (acc_query, pl.ds(0, block))
            query_target = (dq, rows) if j == tiles - 1 else (acc_query, pl.ds(0, block))
            sources = []
            targets = []
            for n, acc in enumerate((acc_key, acc_value)):
                if i > 0:
                    sources.append((acc, held))
                else:
                    sources.append(None if first else (prior[n], held))
                if i < per_shard - 1:
                    targets.append((acc, held))
                elif last:
                    targets.append((outs[n + 2 * side], cols))
                else:
                    targets.append((outs[n], held))
            bit = tile_bit(bits, i * tiles + j)

            @pl.when(bit)
            def _():
                g, q = grad[rows, :], query[rows, :]
                weights = jnp.exp2(scores[held, rows] - norm_i)
                slope = (weights * (probs[held, rows] - dots_i)).astype(jnp.bfloat16)
                settle(
                    True,
                    targets[1],
                    sources[1],
                    lambda: contract(weights.astype(jnp.bfloat16), g, 1, 0),
                )
                settle(True, targets[0], sources[0], lambda: contract(slope, q, 1, 0))
                settle(
                    True,
                    query_target,
                    query_source,
                    lambda: contract(slope, keys[side][cols, :], 0, 0),
                )

            @pl.when(jnp.logical_not(bit))
            def _():
                settle(False, targets[1], sources[1], None)
                settle(False, targets[0], sources[0], None)
                settle(False, query_target, query_source, None)


def split_values(dv, dv_in, keep, send):
    head = lax.axis_index("head")
    member = lax.rem(head, MINOR)
    piece = keep.shape[1]
    for g in range(keep.shape[0]):
        for out, m in ((keep, member), (send, member ^ 1)):
            rows = pl.ds(pl.multiple_of((g * MINOR + m) * piece, piece), piece)
            total = dv[rows, :] + dv_in[rows, :].astype(jnp.float32)
            out[g] = total.astype(out.dtype)


def split_keys(scaling, steps, dk, dk_in, *outs):
    group = lax.axis_index("head") // MINOR
    rows_each = outs[0].shape[0]
    for step, out in zip([0] + steps, outs):
        rows = pl.ds(pl.multiple_of((group ^ step) * rows_each, rows_each), rows_each)
        total = (dk[rows, :] + dk_in[rows, :].astype(jnp.float32)) * scaling
        out[...] = total.astype(out.dtype)


def values_body(steps, value_keep, value_in, *outs):
    group = lax.axis_index("head") // MINOR
    for step, out in zip([0] + steps, outs):
        total = value_keep[group ^ step] + value_in[group ^ step].astype(jnp.float32)
        out[...] = total.astype(out.dtype)


def by_row(row_count, steps, terms):
    head = lax.axis_index("head")
    rows = []
    for r in range(row_count):
        total = None
        for step, term in zip([0] + steps, terms):
            term = term[...].astype(jnp.float32)
            if row_count > 1:
                term = jnp.where((head ^ (step * MINOR)) // HEAD_COUNT == r, term, 0.0)
            total = term if total is None else total + term
        rows.append(total)
    return rows


def keys_body(row_count, steps, *refs):
    terms, (keep, send) = refs[:-2], refs[-2:]
    member = lax.rem(lax.axis_index("head"), MINOR)
    piece = keep.shape[1]
    for r, total in enumerate(by_row(row_count, steps, terms)):
        first, second = total[:piece], total[piece:]
        keep[r] = jnp.where(member == 0, first, second)
        send[r] = jnp.where(member == 0, second, first).astype(send.dtype)


def finish_body(row_count, steps, key_mine, key_in, *refs):
    terms, (grad_keys, grad_values) = refs[:-2], refs[-2:]
    grad_keys[...] = key_mine[...] + key_in[...].astype(jnp.float32)
    for r, total in enumerate(by_row(row_count, steps, terms)):
        grad_values[r] = total


def major_steps(heads):
    major = heads // MINOR
    return sorted(range(1, major), key=lambda step: (-(step & (major // 2)), step))


SMEM = pl.BlockSpec(memory_space=pltpu.SMEM)
VMEM = pl.BlockSpec(memory_space=pltpu.VMEM)


def shift(x, axis, amount):
    size = lax.axis_size(axis)
    return lax.ppermute(x, axis, [(i, (i - amount) % size) for i in range(size)])


def swap(x, bits):
    size = lax.axis_size("head")
    return lax.ppermute(x, "head", [(i, i ^ bits) for i in range(size)])


def swap_cores(x):
    return lax.ppermute(x, "seq", [(i, i ^ 1) for i in range(lax.axis_size("seq"))])


def kernel(body, operands, outs, flops, scratch=()):
    return pl.pallas_call(
        body,
        out_shape=outs,
        in_specs=[SMEM if x.dtype == jnp.int32 and x.ndim < 2 else VMEM for x in operands],
        out_specs=[VMEM] * len(outs),
        scratch_shapes=list(scratch),
        compiler_params=pltpu.CompilerParams(vmem_limit_bytes=VMEM_LIMIT),
        cost_estimate=pl.CostEstimate(
            flops=int(flops), bytes_accessed=int(flops) // 256, transcendentals=0
        ),
    )(*operands)


def gradients(queries, keys, values, d_out, doc_lengths, fold_order):
    local, width = queries.shape[1:]
    chips = lax.axis_size("seq") // CORES
    heads = lax.axis_size("head")
    major = heads // MINOR
    row_count = keys.shape[0]
    piece = local // heads
    block = local // (fold_order.shape[0] // lax.axis_size("seq"))
    tiles = (local // block) * (CORES * local // block)
    scaling = width ** (-0.5)
    factor = scaling * math.log2(math.e)
    row_index = lax.axis_index("head") // HEAD_COUNT
    full = jnp.float32
    low = jnp.bfloat16
    shape = jax.ShapeDtypeStruct

    sets = [(queries[0], d_out[0])]
    for offset in range(1, chips):
        sets.append(
            (shift(queries[0], "seq", offset * CORES), shift(d_out[0], "seq", offset * CORES))
        )
    if row_count == 1:
        key_own, value_own = keys[0], values[0]
    else:
        key_own = lax.dynamic_index_in_dim(keys, row_index, 0, keepdims=False)
        value_own = lax.dynamic_index_in_dim(values, row_index, 0, keepdims=False)
    key_sib, value_sib = swap_cores(key_own), swap_cores(value_own)
    own_arrays = (*sets[0], key_own, value_own)
    places = pl.pallas_call(
        functools.partial(place_body, local),
        out_shape=[shape((local, width), low)] * 4
        + [shape((2 * tiles, block), jnp.int32), shape((8, 128), jnp.int32)] * chips,
        in_specs=[SMEM] * 2 + [VMEM] * 4,
        out_specs=[VMEM] * (4 + 2 * chips),
        name="place",
        compiler_params=pltpu.CompilerParams(vmem_limit_bytes=VMEM_LIMIT),
        cost_estimate=pl.CostEstimate(flops=1 << 20, bytes_accessed=1 << 14, transcendentals=0),
    )(doc_lengths, fold_order, *own_arrays)
    sets[0] = tuple(places[:2])
    key_own, value_own = places[2:4]
    places = places[4:]

    work = 4 * local * CORES * local * width
    stats, held = [], []
    for offset in range(chips):
        info, word = places[2 * offset : 2 * offset + 2]
        pairs = shape((CORES * local, local), full)
        part, scores, probs = kernel(
            functools.partial(stats_body, factor),
            (info, word, *sets[offset], key_own, key_sib, value_own, value_sib),
            [shape((3, local), full), pairs, pairs],
            work,
        )
        stats.append(part)
        held.append((word, scores, probs))
    far = {
        (step, offset): shift(stats[(offset - step) % chips], "seq", step * CORES)
        for step in range(1, chips)
        for offset in range(chips)
    }
    acc = ()
    partial_queries = [None] * chips
    for n, offset in enumerate(list(range(1, chips)) + [0]):
        first, last = n == 0, n == chips - 1
        parts = [stats[offset]] + [far[step, offset] for step in range(1, chips)]
        mine, sent = shape((local, width), full), shape((local, width), low)
        wide = shape((CORES * local, width), full)
        results = kernel(
            functools.partial(grads_body, chips, first, last),
            (*held[offset], *sets[offset], key_own, key_sib, *parts, *acc),
            [mine if offset == 0 else sent]
            + ([mine, mine, sent, sent] if last else [wide, wide]),
            1.5 * work,
            [pltpu.VMEM((CORES * local, width), full)] * 2 + [pltpu.VMEM((block, width), full)],
        )
        partial_queries[offset] = results[0]
        acc = results[1:]
    dk, dv, dk_out, dv_out = acc
    dv_in = swap_cores(dv_out)
    dk_in = swap_cores(dk_out)
    grad_query = partial_queries[0]
    for offset in range(1, chips):
        grad_query = grad_query + shift(
            partial_queries[offset], "seq", -offset * CORES
        ).astype(full)
    grad_queries = (grad_query * scaling).astype(low)[None]

    tail = 4 * local * width
    steps = major_steps(heads)
    value_keep, value_send = kernel(
        split_values,
        (dv, dv_in),
        [shape((major, piece, width), full), shape((major, piece, width), low)],
        tail,
    )
    value_in = swap(value_send, 1)
    key_keep, *key_send = kernel(
        functools.partial(split_keys, scaling, steps),
        (dk, dk_in),
        [shape((MINOR * piece, width), full)]
        + [shape((MINOR * piece, width), low)] * (major - 1),
        tail,
    )
    key_terms = [key_keep]
    for step, x in zip(steps, key_send):
        key_terms.append(swap(x, step * MINOR))
    value_mine, *value_out = kernel(
        functools.partial(values_body, steps),
        (value_keep, value_in),
        [shape((piece, width), full)] + [shape((piece, width), low)] * (major - 1),
        tail,
    )
    value_terms = [value_mine]
    for step, x in zip(steps, value_out):
        value_terms.append(swap(x, step * MINOR))
    owned = (row_count, piece, width)
    key_mine, key_out = kernel(
        functools.partial(keys_body, row_count, steps),
        key_terms,
        [shape(owned, full), shape(owned, low)],
        tail,
    )
    key_in = swap(key_out, 1)
    grad_keys, grad_values = kernel(
        functools.partial(finish_body, row_count, steps),
        (key_mine, key_in, *value_terms),
        [shape(owned, full)] * 2,
        tail,
    )
    return grad_queries, grad_keys, grad_values


def solution(mesh):
    in_specs = (
        P("head", "seq", None),
        P(None, "seq", None),
        P(None, "seq", None),
        P("head", "seq", None),
        P(),
        P(),
    )
    out_specs = (
        P("head", "seq", None),
        P(None, ("seq", "head"), None),
        P(None, ("seq", "head"), None),
    )
    return jax.shard_map(
        gradients, mesh=mesh, in_specs=in_specs, out_specs=out_specs, check_vma=False
    )
```

```python
import functools
import math

import jax
import jax.numpy as jnp
from jax import lax
from jax.experimental import pallas as pl
from jax.experimental.pallas import tpu as pltpu
from jax.sharding import PartitionSpec as P


HEAD_COUNT = 8
MASKED = -1e30
VMEM_LIMIT = 14 * 1024 * 1024
CORES = 2
MINOR = 2


def contract(left, right, left_dim, right_dim):
    return lax.dot_general(
        left, right, (((left_dim,), (right_dim,)), ((), ())), preferred_element_type=jnp.float32
    )


def place_body(local, docs, fold, *refs):
    for source, target in zip(refs[:4], refs[4:8]):
        target[...] = source[...]
    outs = refs[8:]
    seq_total = lax.axis_size("seq")
    per_shard = fold.shape[0] // seq_total
    block = local // per_shard
    own = lax.axis_index("seq")
    row = lax.axis_index("head") // HEAD_COUNT
    starts = [jnp.int32(0)]
    for d in range(docs.shape[1] - 1):
        starts.append(starts[-1] + docs[row, d])
    key_bases = [
        fold[shard * per_shard + j] * block for shard in (own, own ^ 1) for j in range(per_shard)
    ]
    for offset in range(len(outs) // 2):
        info, word = outs[2 * offset : 2 * offset + 2]
        shard = lax.rem(own + offset * CORES, seq_total)
        bits = jnp.int32(0)
        for i in range(per_shard):
            base = fold[shard * per_shard + i] * block
            position = base + lax.broadcasted_iota(jnp.int32, (1, block), 1)
            start = jnp.zeros((1, block), jnp.int32)
            first = jnp.int32(0)
            for d in starts[1:]:
                start = jnp.where(position >= d, d, start)
                first = jnp.where(base >= d, d, first)
            for j, key_base in enumerate(key_bases):
                tile = i * len(key_bases) + j
                info[2 * tile : 2 * tile + 1, :] = start - key_base
                info[2 * tile + 1 : 2 * tile + 2, :] = position - key_base
                active = (key_base <= base) & (key_base + block > first)
                bits = bits | jnp.where(active, 1 << tile, 0)
        word[...] = jnp.full(word.shape, bits, jnp.int32)


def tile_bit(bits, tile):
    return ((bits >> tile) & 1) == 1


def allowed_scores(factor, info, tile, key_index, keys, query):
    allowed = (key_index >= info[2 * tile : 2 * tile + 1, :]) & (
        key_index <= info[2 * tile + 1 : 2 * tile + 2, :]
    )
    return jnp.where(allowed, contract(keys, query, 1, 1) * factor, MASKED)


def stats_body(factor, info, word, query, *refs):
    keys = refs[0:2]
    whole = len(refs) == 8
    if whole:
        grad, values, (out, scores_out, prob_out) = refs[2], refs[3:5], refs[5:]
    else:
        out, scores_out = refs[2:]
    local = query.shape[0]
    block = info.shape[1]
    per_shard = local // block
    bits = jnp.max(word[...])
    key_index = lax.broadcasted_iota(jnp.int32, (block, block), 0)
    for i in range(per_shard):
        rows = pl.ds(i * block, block)
        out[0:1, rows] = jnp.full((1, block), MASKED, jnp.float32)
        out[1:, rows] = jnp.zeros((out.shape[0] - 1, block), jnp.float32)
        for j in range(CORES * per_shard):
            tile = i * CORES * per_shard + j
            side, cols = j // per_shard, pl.ds(j % per_shard * block, block)
            held = pl.ds(j * block, block)

            @pl.when(tile_bit(bits, tile))
            def _():
                scores = allowed_scores(
                    factor, info, tile, key_index, keys[side][cols, :], query[rows, :]
                )
                scores_out[held, rows] = scores
                old_max = out[0:1, rows]
                new_max = jnp.maximum(old_max, jnp.max(scores, axis=0, keepdims=True))
                keep = jnp.exp2(old_max - new_max)
                weights = jnp.exp2(scores - new_max)
                out[0:1, rows] = new_max
                out[1:2, rows] = out[1:2, rows] * keep + jnp.sum(weights, axis=0, keepdims=True)
                if whole:
                    prob = contract(values[side][cols, :], grad[rows, :], 1, 1)
                    prob_out[held, rows] = prob
                    out[2:3, rows] = out[2:3, rows] * keep + jnp.sum(
                        weights * prob, axis=0, keepdims=True
                    )


def copy_body(source, target):
    target[...] = source[...]


def dots_body(per_shard, word, scores, sums, grad, value_own, value_sib, out, prob_out):
    local = grad.shape[0]
    block = local // per_shard
    bits = jnp.max(word[...])
    for i in range(per_shard):
        rows = pl.ds(i * block, block)
        out[:, rows] = jnp.zeros((1, block), jnp.float32)
        for j in range(CORES * per_shard):
            cols, held = pl.ds(j % per_shard * block, block), pl.ds(j * block, block)
            values = (value_own, value_sib)[j // per_shard]

            @pl.when(tile_bit(bits, i * CORES * per_shard + j))
            def _():
                prob = contract(values[cols, :], grad[rows, :], 1, 1)
                prob_out[held, rows] = prob
                weights = jnp.exp2(scores[held, rows] - sums[0:1, rows])
                out[:, rows] += jnp.sum(weights * prob, axis=0, keepdims=True)


def row_norm(sums):
    top = sums[0][0:1, :]
    for part in sums[1:]:
        top = jnp.maximum(top, part[0:1, :])
    total = jnp.zeros_like(top)
    for part in sums:
        total = total + part[1:2, :] * jnp.exp2(part[0:1, :] - top)
    return top + jnp.log2(total)


def row_dots(sums, dots, norm):
    whole = jnp.zeros_like(norm)
    for part, dot in zip(sums, dots):
        whole = whole + dot[dot.shape[0] - 1 :, :] * jnp.exp2(part[0:1, :] - norm)
    return whole


def add_up(target, sources, term):
    ref, at = target
    value = jnp.zeros((at.size, ref.shape[1]), jnp.float32)
    for written, source, where in reversed(sources):
        value = jnp.where(written, source[where, :].astype(jnp.float32), value)
    ref[at, :] = (value if term is None else value + term()).astype(ref.dtype)


def any_of(flags):
    return functools.reduce(jnp.logical_or, flags)


def values_body(parts, per_shard, sets, *refs):
    refs = list(refs)
    groups = []
    for _ in range(sets):
        word, scores, grad = refs[:3]
        groups.append((jnp.max(word[...]), scores, grad, row_norm(refs[3 : 3 + parts])))
        refs = refs[3 + parts :]
    mine, sent, acc = refs
    block = mine.shape[0] // per_shard
    tiles = CORES * per_shard
    count = sets * per_shard
    for j in range(tiles):
        held, cols = pl.ds(j * block, block), pl.ds(j % per_shard * block, block)
        flags = [tile_bit(groups[n // per_shard][0], n % per_shard * tiles + j) for n in range(count)]
        for n in range(count):
            _, scores, grad, norm = groups[n // per_shard]
            i = n % per_shard
            rows = pl.ds(i * block, block)
            norm_i = norm[:, i * block : (i + 1) * block]
            sources = [(any_of(flags[:n]), acc, held)] if n else []
            ends = n == count - 1
            target = ((mine, sent)[j // per_shard], cols) if ends else (acc, held)

            @pl.when(flags[n])
            def _():
                weights = jnp.exp2(scores[held, rows] - norm_i).astype(jnp.bfloat16)
                add_up(target, sources, lambda: contract(weights, grad[rows, :], 1, 0))

            if ends:

                @pl.when(jnp.logical_not(flags[n]))
                def _():
                    add_up(target, sources, None)


def keys_grads_body(parts, per_shard, first, last, word, scores, probs, query, *refs):
    keys = refs[0:2]
    sums, dots = refs[2 : 2 + parts], refs[2 + parts : 2 + 2 * parts]
    refs = refs[2 + 2 * parts :]
    if not first:
        prior, prior_word, *refs = refs
        prior_bits = jnp.max(prior_word[...])
    dq, outs, (acc, acc_query) = refs[0], refs[1:-2], refs[-2:]
    block = query.shape[0] // per_shard
    tiles = CORES * per_shard
    bits = jnp.max(word[...])
    norm = row_norm(sums)
    whole = row_dots(sums, dots, norm)
    flags = [[tile_bit(bits, i * tiles + j) for j in range(tiles)] for i in range(per_shard)]
    first_rows = pl.ds(0, block)
    for i in range(per_shard):
        rows = pl.ds(i * block, block)
        norm_i = norm[:, i * block : (i + 1) * block]
        dots_i = whole[:, i * block : (i + 1) * block]
        for j in range(tiles):
            side, cols = j // per_shard, pl.ds(j % per_shard * block, block)
            held = pl.ds(j * block, block)
            ends = i == per_shard - 1 and not first
            if ends:
                target = (outs[side], cols) if last else (outs[0], held)
            else:
                target = (outs[0] if first else acc, held)
            sources = []
            if i > 0:
                earlier = any_of([flags[e][j] for e in range(i)])
                sources.append((earlier, outs[0] if first else acc, held))
            if not first:
                mask = sum(1 << (e * tiles + j) for e in range(per_shard))
                sources.append(((prior_bits & mask) != 0, prior, held))
            query_ends = j == tiles - 1
            query_target = (dq, rows) if query_ends else (acc_query, first_rows)
            query_sources = [(any_of(flags[i][:j]), acc_query, first_rows)] if j else []

            @pl.when(flags[i][j])
            def _():
                weights = jnp.exp2(scores[held, rows] - norm_i)
                slope = (weights * (probs[held, rows] - dots_i)).astype(jnp.bfloat16)
                add_up(target, sources, lambda: contract(slope, query[rows, :], 1, 0))
                add_up(
                    query_target,
                    query_sources,
                    lambda: contract(slope, keys[side][cols, :], 0, 0),
                )

            if ends or query_ends:

                @pl.when(jnp.logical_not(flags[i][j]))
                def _():
                    if ends:
                        add_up(target, sources, None)
                    if query_ends:
                        add_up(query_target, query_sources, None)


def split_values(dv, dv_in, keep, send):
    head = lax.axis_index("head")
    member = lax.rem(head, MINOR)
    piece = keep.shape[1]
    for g in range(keep.shape[0]):
        for out, m in ((keep, member), (send, member ^ 1)):
            rows = pl.ds(pl.multiple_of((g * MINOR + m) * piece, piece), piece)
            total = dv[rows, :] + dv_in[rows, :].astype(jnp.float32)
            out[g] = total.astype(out.dtype)


def split_keys(scaling, steps, dk, dk_in, *outs):
    group = lax.axis_index("head") // MINOR
    rows_each = outs[0].shape[0]
    for step, out in zip([0] + steps, outs):
        rows = pl.ds(pl.multiple_of((group ^ step) * rows_each, rows_each), rows_each)
        total = (dk[rows, :] + dk_in[rows, :].astype(jnp.float32)) * scaling
        out[...] = total.astype(out.dtype)


def minor_body(steps, value_keep, value_in, *outs):
    group = lax.axis_index("head") // MINOR
    for step, out in zip([0] + steps, outs):
        total = value_keep[group ^ step] + value_in[group ^ step].astype(jnp.float32)
        out[...] = total.astype(out.dtype)


def by_row(row_count, steps, terms):
    head = lax.axis_index("head")
    rows = []
    for r in range(row_count):
        total = None
        for step, term in zip([0] + steps, terms):
            term = term[...].astype(jnp.float32)
            if row_count > 1:
                term = jnp.where((head ^ (step * MINOR)) // HEAD_COUNT == r, term, 0.0)
            total = term if total is None else total + term
        rows.append(total)
    return rows


def keys_body(row_count, steps, *refs):
    terms, (keep, send) = refs[:-2], refs[-2:]
    member = lax.rem(lax.axis_index("head"), MINOR)
    piece = keep.shape[1]
    for r, total in enumerate(by_row(row_count, steps, terms)):
        first, second = total[:piece], total[piece:]
        keep[r] = jnp.where(member == 0, first, second)
        send[r] = jnp.where(member == 0, second, first).astype(send.dtype)


def finish_body(row_count, steps, key_mine, key_in, *refs):
    terms, (grad_keys, grad_values) = refs[:-2], refs[-2:]
    grad_keys[...] = key_mine[...] + key_in[...].astype(jnp.float32)
    for r, total in enumerate(by_row(row_count, steps, terms)):
        grad_values[r] = total


def major_steps(heads):
    major = heads // MINOR
    return sorted(range(1, major), key=lambda step: (-(step & (major // 2)), step))


SMEM = pl.BlockSpec(memory_space=pltpu.SMEM)
VMEM = pl.BlockSpec(memory_space=pltpu.VMEM)


def shift(x, axis, amount):
    size = lax.axis_size(axis)
    return lax.ppermute(x, axis, [(i, (i - amount) % size) for i in range(size)])


def swap(x, bits):
    size = lax.axis_size("head")
    return lax.ppermute(x, "head", [(i, i ^ bits) for i in range(size)])


def swap_cores(x):
    return lax.ppermute(x, "seq", [(i, i ^ 1) for i in range(lax.axis_size("seq"))])


def kernel(body, operands, outs, flops, scratch=()):
    return pl.pallas_call(
        body,
        out_shape=outs,
        in_specs=[SMEM if x.dtype == jnp.int32 and x.ndim < 2 else VMEM for x in operands],
        out_specs=[VMEM] * len(outs),
        scratch_shapes=list(scratch),
        compiler_params=pltpu.CompilerParams(vmem_limit_bytes=VMEM_LIMIT),
        cost_estimate=pl.CostEstimate(
            flops=int(flops), bytes_accessed=int(flops) // 256, transcendentals=0
        ),
    )(*operands)


def gradients(queries, keys, values, d_out, doc_lengths, fold_order):
    local, width = queries.shape[1:]
    chips = lax.axis_size("seq") // CORES
    heads = lax.axis_size("head")
    major = heads // MINOR
    row_count = keys.shape[0]
    piece = local // heads
    block = local // (fold_order.shape[0] // lax.axis_size("seq"))
    tiles = (local // block) * (CORES * local // block)
    scaling = width ** (-0.5)
    factor = scaling * math.log2(math.e)
    row_index = lax.axis_index("head") // HEAD_COUNT
    full = jnp.float32
    low = jnp.bfloat16
    shape = jax.ShapeDtypeStruct

    sets = [(queries[0], d_out[0])]
    for offset in range(1, chips):
        query = shift(queries[0], "seq", offset * CORES)
        grad = shift(d_out[0], "seq", offset * CORES)
        sets.append((query, grad))
    if row_count == 1:
        key_own, value_own = keys[0], values[0]
    else:
        key_own = lax.dynamic_index_in_dim(keys, row_index, 0, keepdims=False)
        value_own = lax.dynamic_index_in_dim(values, row_index, 0, keepdims=False)
    key_sib, value_sib = swap_cores(key_own), swap_cores(value_own)
    own_arrays = (*sets[0], key_own, value_own)
    places = pl.pallas_call(
        functools.partial(place_body, local),
        out_shape=[shape((local, width), low)] * 4
        + [shape((2 * tiles, block), jnp.int32), shape((8, 128), jnp.int32)] * chips,
        in_specs=[SMEM] * 2 + [VMEM] * 4,
        out_specs=[VMEM] * (4 + 2 * chips),
        name="place",
        compiler_params=pltpu.CompilerParams(vmem_limit_bytes=VMEM_LIMIT),
        cost_estimate=pl.CostEstimate(flops=1 << 20, bytes_accessed=1 << 14, transcendentals=0),
    )(doc_lengths, fold_order, *own_arrays)
    sets[0] = tuple(places[:2])
    key_own, value_own = places[2:4]
    places = places[4:]

    work = 4 * local * CORES * local * width
    per_shard = local // block
    mine, sent = shape((local, width), full), shape((local, width), low)
    wide = shape((CORES * local, width), full)
    pairs = shape((CORES * local, local), full)
    words, sums, dots, scores, probs = [], [], [], [], []
    for offset in range(chips):
        info, word = places[2 * offset : 2 * offset + 2]
        query, grad = sets[offset]
        own = offset == 0
        results = kernel(
            functools.partial(stats_body, factor),
            (info, word, query, key_own, key_sib)
            + ((grad, value_own, value_sib) if own else ()),
            [shape((3 if own else 2, local), full)] + [pairs] * (2 if own else 1),
            work if own else work // 2,
        )
        words.append(word)
        sums.append(results[0])
        scores.append(results[1])
        if own:
            dots.append(results[0])
            probs.append(results[2])
    far_sums, far_dots = {}, {}
    for offset in range(chips):
        for step in range(1, chips):
            far_sums[step, offset] = shift(
                sums[(offset - step) % chips], "seq", step * CORES
            )
    for offset in range(1, chips):
        (words[offset],) = kernel(
            copy_body, (words[offset],), [shape(words[offset].shape, jnp.int32)], 1024
        )
    for offset in range(1, chips):
        dot, prob = kernel(
            functools.partial(dots_body, per_shard),
            (words[offset], scores[offset], sums[offset], sets[offset][1])
            + (value_own, value_sib),
            [shape((1, local), full), pairs],
            work // 2,
        )
        dots.append(dot)
        probs.append(prob)
    for offset in range(chips):
        for step in range(1, chips):
            if offset == step:
                far_dots[step, offset] = far_sums[step, offset]
                continue
            far_dots[step, offset] = shift(
                dots[(offset - step) % chips], "seq", step * CORES
            )
    all_sums = [
        (sums[offset], *(far_sums[step, offset] for step in range(1, chips)))
        for offset in range(chips)
    ]
    all_dots = [
        (dots[offset], *(far_dots[step, offset] for step in range(1, chips)))
        for offset in range(chips)
    ]
    operands = ()
    for offset in range(chips):
        operands += (words[offset], scores[offset], sets[offset][1], *all_sums[offset])
    dv, dv_out = kernel(
        functools.partial(values_body, chips, per_shard, chips),
        operands,
        [mine, sent],
        work // 2,
        [pltpu.VMEM((CORES * local, width), full)],
    )
    acc = ()
    partial_queries = [None] * chips
    for n, offset in enumerate(list(range(1, chips)) + [0]):
        first, last = n == 0, n == chips - 1
        partial_queries[offset], *acc = kernel(
            functools.partial(keys_grads_body, chips, per_shard, first, last),
            (words[offset], scores[offset], probs[offset], sets[offset][0])
            + (key_own, key_sib, *all_sums[offset], *all_dots[offset], *acc),
            [mine if offset == 0 else sent] + ([mine, sent] if last else [wide]),
            work,
            [pltpu.VMEM((CORES * local, width), full), pltpu.VMEM((block, width), full)],
        )
        if not last:
            acc.append(words[offset] if first else jnp.full_like(words[offset], -1))
    dk, dk_out = acc
    dv_in = swap_cores(dv_out)
    dk_in = swap_cores(dk_out)
    grad_query = partial_queries[0]
    for offset in range(1, chips):
        grad_query = grad_query + shift(
            partial_queries[offset], "seq", -offset * CORES
        ).astype(full)
    grad_queries = (grad_query * scaling).astype(low)[None]

    tail = 4 * local * width
    steps = major_steps(heads)
    value_keep, value_send = kernel(
        split_values,
        (dv, dv_in),
        [shape((major, piece, width), full), shape((major, piece, width), low)],
        tail,
    )
    value_in = swap(value_send, 1)
    key_keep, *key_send = kernel(
        functools.partial(split_keys, scaling, steps),
        (dk, dk_in),
        [shape((MINOR * piece, width), full)]
        + [shape((MINOR * piece, width), low)] * (major - 1),
        tail,
    )
    key_terms = [key_keep]
    for step, x in zip(steps, key_send):
        key_terms.append(swap(x, step * MINOR))
    value_mine, *value_out = kernel(
        functools.partial(minor_body, steps),
        (value_keep, value_in),
        [shape((piece, width), full)] + [shape((piece, width), low)] * (major - 1),
        tail,
    )
    value_terms = [value_mine]
    for step, x in zip(steps, value_out):
        value_terms.append(swap(x, step * MINOR))
    owned = (row_count, piece, width)
    key_mine, key_out = kernel(
        functools.partial(keys_body, row_count, steps),
        key_terms,
        [shape(owned, full), shape(owned, low)],
        tail,
    )
    key_in = swap(key_out, 1)
    grad_keys, grad_values = kernel(
        functools.partial(finish_body, row_count, steps),
        (key_mine, key_in, *value_terms),
        [shape(owned, full)] * 2,
        tail,
    )
    return grad_queries, grad_keys, grad_values


def solution(mesh):
    in_specs = (
        P("head", "seq", None),
        P(None, "seq", None),
        P(None, "seq", None),
        P("head", "seq", None),
        P(),
        P(),
    )
    out_specs = (
        P("head", "seq", None),
        P(None, ("seq", "head"), None),
        P(None, ("seq", "head"), None),
    )
    return jax.shard_map(
        gradients, mesh=mesh, in_specs=in_specs, out_specs=out_specs, check_vma=False
    )
```
